768 devices in a mesh: dp: 48 (over y_lo, z), section: 8 (over x, core), tensor: 2 (over y_hi).
Axes of the slice: x: 4, y: 8 (y_hi: 2, y_lo: 4; y = y_hi * 4 + y_lo), z: 12, core: 2. Of those that a mesh axis runs over, the one named last changes fastest.
Arguments:
- hidden: bfloat16 [18432, 8192], P(('dp', 'section', 'tensor')), may hold values from -6 to 6
- proj_weight: bfloat16 [8192, 8192], P(None, ('section', 'tensor')), may hold values from -0.0625 to 0.0625
- proj_bias: bfloat16 [8192], P(('section', 'tensor')), may hold values from -3 to 3
- route: int32 [18432, 1], P(('dp', 'section', 'tensor')), may hold values from 0 to 47; in each aligned block of 24 rows (0 to 23, 24 to 47, ...) at most 2 rows name the same one
- text: bfloat16 [73728, 8192], P(('dp', 'section', 'tensor')), may hold values from -6 to 6
- norm_gain: bfloat16 [8192], replicated, may hold values from 0.5 to 1.5
Outputs:
- normed: bfloat16 [73728, 8192], P(('dp', 'section', 'tensor'))
The draws below stay inside these ranges and needn't reach their ends.
Inputs may be any that keep to these rules, and one draw needn't show every extreme that they name: `route`: among the rows of one device no replica is named more than 2 times; some device reaches 2.
All inputs are finite; a program needn't handle non-finite values.
Results may differ from the reference program's by a relative error of at most 0.0031.
Values may be sent and summed in bfloat16 or wider, within the bound.
No kernel may reach another device: no remote copies, remote signals or barrier semaphores. Data moves between devices by JAX's collectives and lax.ppermute only.
A program may use at most 64 MiB of HBM per device.

```python
import math
import jax
import jax.numpy as jnp
import numpy as np
from jax import lax

D = 8192
TOK_DEV = 24
CAP = 2
SEQ_DEV = 96
TOKENS = 18432
ROWS = 73728
N_DP = 48
N_SECTION = 8
N_TENSOR = 2


def level_of(stream_key, shape, pieces, smallest, largest):
    factor_of, own = 1.0, jax.random.fold_in(stream_key, 6)
    for axis_at, blocks in pieces:
        heights = jnp.exp(jax.random.uniform(jax.random.fold_in(own, axis_at), (blocks,), jnp.float32, smallest / len(pieces), largest / len(pieces)))
        factor_of = factor_of * jnp.repeat(heights, shape[axis_at] // blocks).reshape([-1 if axis == axis_at else 1 for axis in range(len(shape))])
    return factor_of


def assign_block(stream_key, own, number, rows, count, top, most, lean):
    sequence = jax.random.permutation(stream_key, count)
    crowded, common = shares(count, rows * top, most, lean, True), shares(count, rows * top, most, lean, False)
    places = jnp.arange(count)

    def named(lengths, rotation):
        used = int((lengths > 0).sum())
        fixed = max(1, used // 4)
        moved = fixed + (places - fixed + rotation * (used - fixed)) % max(1, count - fixed)
        return jnp.zeros((count,), jnp.int32).at[sequence[jnp.where(places < fixed, places, moved)]].set(jnp.asarray(lengths, jnp.int32))

    lengths = jnp.where(number % 4 == 0, named(crowded, number // 4), named(common, number - number // 4 - 1))
    mixed = jax.random.permutation(jax.random.fold_in(own, 3), count)
    donor, taker = mixed[0:count // 2 * 2:2], mixed[1:count // 2 * 2:2]
    room = jnp.minimum(lengths[donor] - 1, most - lengths[taker]) // 2
    room = jnp.where((donor == sequence[0]) | (taker == sequence[0]) | (lengths[taker] == 0), 0, jnp.maximum(room, 0))
    moved = jax.random.randint(jax.random.fold_in(own, 4), (count // 2,), 0, 1 << 20) % (room + 1)
    lengths = lengths.at[donor].add(-moved).at[taker].add(moved)
    labels = jnp.searchsorted(jnp.cumsum(lengths), jnp.arange(rows * top), side="right").astype(jnp.int32)
    grid = labels.reshape(top, rows).T
    grid = grid[jax.random.permutation(jax.random.fold_in(own, 1), rows)]
    rotation = jax.random.randint(jax.random.fold_in(own, 2), (rows, 1), 0, top)
    return jnp.take_along_axis(grid, (jnp.arange(top)[None, :] + rotation) % top, axis=1)


def shares(amount, total, most, skew, full):
    weights = [(1 << 20) // math.isqrt(rank ** skew) + 1 for rank in range(1, amount + 1)]
    largest = most if full else min(most, max(-(-total // amount), total * weights[0] // sum(weights)))
    least = 1 if total - largest >= amount - 1 else 0
    counts, spare = [largest] + [least] * (amount - 1), total - largest - least * (amount - 1)
    while spare > 0:
        movable = [i for i in range(1, amount) if counts[i] < largest] or [i for i in range(1, amount) if counts[i] < most]
        pool, left = sum([weights[i] for i in movable]), spare
        for i in movable:
            addition = min(most - counts[i], max(1, left * weights[i] // pool), spare)
            counts[i] = counts[i] + addition
            spare = spare - addition
    return np.array(counts)


def centred(key, dims, scale, most, shards=(), kind=jnp.bfloat16):
    entries = jax.random.normal(key, dims, jnp.float32) * scale
    if len(shards) > 0:
        entries = level_of(key, dims, shards, -0.22, 0.18) * entries
    return jnp.clip(entries, min=-most, max=most).astype(kind)


def setup_inputs(seed: int = 0) -> dict:
    arg_keys = jax.random.split(jax.random.key(seed), 7)
    hidden = centred(arg_keys[0], (TOKENS, D), 1.0, 6.0, ((0, 768),))
    proj_weight = centred(arg_keys[1], (D, D), D ** -0.5, 0.0625, ((1, 16),))
    proj_bias = centred(arg_keys[2], (D,), 0.5, 3.0, ((0, 16),))
    route_keys = jax.random.split(jax.random.fold_in(arg_keys[3], 1), TOKENS // TOK_DEV)
    route_turns = jax.random.permutation(jax.random.fold_in(arg_keys[3], 3), TOKENS // TOK_DEV)
    route = jax.vmap(lambda own, number: assign_block(jax.random.fold_in(arg_keys[3], 2), own, number, TOK_DEV, N_DP, 1, CAP, 2))(route_keys, route_turns).reshape((TOKENS, 1))
    text = centred(arg_keys[4], (ROWS, D), 1.0, 6.0, ((0, 768),))
    norm_gain = jnp.clip(1.0 + 0.1 * jax.random.normal(arg_keys[5], (D,), jnp.float32), 0.5, 1.5).astype(jnp.bfloat16)
    return dict(hidden=hidden, proj_weight=proj_weight, proj_bias=proj_bias, route=route, text=text, norm_gain=norm_gain)


def reference(hidden, proj_weight, proj_bias, route, text, norm_gain):
    groups = N_SECTION * N_TENSOR
    projected = (jnp.dot(hidden, proj_weight, preferred_element_type=jnp.float32) + proj_bias.astype(jnp.float32)).astype(jnp.bfloat16)
    width = projected.shape[1]
    grouped = projected.reshape(N_DP, groups, TOK_DEV, width).transpose(1, 0, 2, 3).reshape(groups, N_DP * TOK_DEV, width)
    target = route[:, 0].astype(jnp.int32).reshape(N_DP, groups, TOK_DEV).transpose(1, 0, 2).reshape(groups, N_DP * TOK_DEV)
    onehot = (target[:, :, None] == jnp.arange(N_DP, dtype=jnp.int32)[None, None, :]).astype(jnp.int32)
    running = jnp.cumsum(onehot, axis=1).astype(jnp.int32)
    position = (lax.optimization_barrier(jnp.sum(running * onehot, axis=2)) - 1).astype(jnp.int32)
    group_index = jnp.broadcast_to(jnp.arange(groups, dtype=jnp.int32)[:, None], target.shape)
    base = text.reshape(N_DP, groups, SEQ_DEV, width)
    merged = base.at[target, group_index, position].set(grouped)
    values = merged.astype(jnp.float32)
    scale_inv = lax.rsqrt(lax.optimization_barrier(jnp.mean(values * values, axis=-1, keepdims=True)) + 1e-05)
    normed = (values * scale_inv * norm_gain.astype(jnp.float32)).astype(jnp.bfloat16)
    return normed.reshape(N_DP * groups * SEQ_DEV, width)
```

```python
import functools

import jax
import jax.numpy as jnp
from jax import lax
from jax.experimental import pallas as pl
from jax.experimental.pallas import tpu as pltpu
from jax.sharding import PartitionSpec as P


EMPTY = 2.0**100
NX = 4


def shift_x(block, by):
    n = lax.axis_size("section") // 2
    pairs = [(2 * x + c, 2 * ((x + by) % n) + c) for x in range(n) for c in range(2)]
    return lax.ppermute(block, "section", pairs)


def swap_core(block):
    n = lax.axis_size("section")
    return lax.ppermute(block, "section", [(i, i ^ 1) for i in range(n)])


def project_kernel(partner, lhs_ref, w_ref, bias_ref, *rest):
    out_ref, acc = rest[-2:]
    step = pl.program_id(0)

    @pl.when(step == 0)
    def _():
        acc[...] = jnp.zeros_like(acc)
        if partner:
            out_ref[...] = rest[0][...]

    acc[...] += jnp.dot(lhs_ref[...], w_ref[...], preferred_element_type=jnp.float32)

    @pl.when(step == pl.num_programs(0) - 1)
    def _():
        section = lax.axis_index("section")
        tensor = lax.axis_index("tensor")
        x, core = section // 2, section % 2
        t = (1 - tensor) if partner else tensor
        rows = out_ref.shape[1]
        bias = bias_ref[...].astype(jnp.float32)
        for k in range(2 * NX):
            c = core if k < NX else 1 - core
            from_x = lax.rem(x - k % NX + NX, NX)
            dst = (from_x * 2 + c) * 2 + t
            out_ref[dst] = (acc[k * rows : (k + 1) * rows, :] + bias).astype(out_ref.dtype)


def project(lhs, weight, bias, partner, base=None):
    rows, depth = lhs.shape
    width = weight.shape[1]
    step = 1024
    count = rows // (2 * NX)
    whole = lambda k: (0, 0, 0)
    specs = [
        pl.BlockSpec((rows, step), lambda k: (0, k)),
        pl.BlockSpec((step, width), lambda k: (k, 0)),
        pl.BlockSpec((1, width), lambda k: (0, 0)),
    ]
    operands = [lhs, weight, bias]
    if base is not None:
        specs.append(pl.BlockSpec((4 * NX, count, width), whole))
        operands.append(base)
    out_spec = pl.BlockSpec((4 * NX, count, width), whole)
    return pl.pallas_call(
        functools.partial(project_kernel, partner),
        grid=(depth // step,),
        in_specs=specs,
        out_specs=out_spec,
        out_shape=jax.ShapeDtypeStruct((4 * NX, count, width), jnp.bfloat16),
        scratch_shapes=[pltpu.VMEM((rows, width), jnp.float32)],
        cost_estimate=pl.CostEstimate(
            flops=2 * rows * depth * width,
            bytes_accessed=2 * (rows * depth + depth * width + rows * width),
            transcendentals=0,
        ),
        name="project_partner" if partner else "project_own",
    )(*operands)


def pack_kernel(route_ref, tokens_ref, out_ref):
    blocks, rows, width = tokens_ref.shape
    slots = out_ref.shape[0]
    first = lax.broadcasted_iota(jnp.int32, (rows, rows), 0)
    second = lax.broadcasted_iota(jnp.int32, (rows, rows), 1)
    down = route_ref[...].astype(jnp.float32)
    across = jnp.sum(jnp.where(first == second, down, 0.0), axis=0, keepdims=True)
    earlier = jnp.where((first < second) & (down == across), 1.0, 0.0)
    slot = 2.0 * across + jnp.sum(earlier, axis=0, keepdims=True)
    ids = lax.broadcasted_iota(jnp.int32, (slots, rows), 0).astype(jnp.float32)
    pick = jnp.where(ids == slot, 1.0, 0.0)
    mark = jnp.where(jnp.sum(pick, axis=1, keepdims=True) > 0.0, 0.0, EMPTY)
    pick = pick.astype(jnp.bfloat16)
    for k in range(blocks):
        moved = jnp.dot(pick, tokens_ref[k], preferred_element_type=jnp.float32)
        out_ref[:, k * width : (k + 1) * width] = (moved + mark).astype(out_ref.dtype)


def pack(route, tokens, slots):
    blocks, rows, width = tokens.shape
    return pl.pallas_call(
        pack_kernel,
        in_specs=[pl.BlockSpec(memory_space=pltpu.VMEM)] * 2,
        out_specs=pl.BlockSpec(memory_space=pltpu.VMEM),
        out_shape=jax.ShapeDtypeStruct((slots, blocks * width), jnp.bfloat16),
        cost_estimate=pl.CostEstimate(
            flops=2 * slots * rows * blocks * width,
            bytes_accessed=2 * (slots + rows) * blocks * width,
            transcendentals=0,
        ),
        name="pack",
    )(route, tokens)


def finish_kernel(inbox_ref, text_ref, gain_ref, out_ref, merged):
    slots, width = inbox_ref.shape
    rows = text_ref.shape[0]
    first = lax.broadcasted_iota(jnp.int32, (slots, slots), 0)
    second = lax.broadcasted_iota(jnp.int32, (slots, slots), 1)
    down = jnp.where(inbox_ref[:, 0:128].astype(jnp.float32)[:, 0:1] < EMPTY / 2, 1.0, 0.0)
    across = jnp.sum(jnp.where(first == second, down, 0.0), axis=0, keepdims=True)
    place = jnp.sum(jnp.where(first < second, down, 0.0), axis=0, keepdims=True)
    ids = lax.broadcasted_iota(jnp.int32, (rows, slots), 0).astype(jnp.float32)
    pick = jnp.where((ids == place) & (across > 0.0), 1.0, 0.0)
    is_image = jnp.sum(pick, axis=1, keepdims=True) > 0.0
    pick = pick.astype(jnp.bfloat16)
    step = 1024
    square = jnp.zeros((rows, 1), jnp.float32)
    for k in range(width // step):
        at = slice(k * step, (k + 1) * step)
        moved = jnp.dot(pick, inbox_ref[:, at], preferred_element_type=jnp.float32)
        values = jnp.where(is_image, moved, text_ref[:, at].astype(jnp.float32))
        merged[:, at] = values
        square += jnp.sum(values * values, axis=1, keepdims=True)
    scale_inv = lax.rsqrt(square * (1.0 / width) + 1e-05)
    for k in range(width // step):
        at = slice(k * step, (k + 1) * step)
        gain = gain_ref[:, at].astype(jnp.float32)
        out_ref[:, at] = (merged[:, at] * scale_inv * gain).astype(out_ref.dtype)


def finish(inbox, text, gain):
    rows, width = text.shape
    return pl.pallas_call(
        finish_kernel,
        in_specs=[pl.BlockSpec(memory_space=pltpu.VMEM)] * 3,
        out_specs=pl.BlockSpec(memory_space=pltpu.VMEM),
        out_shape=jax.ShapeDtypeStruct((rows, width), jnp.bfloat16),
        scratch_shapes=[pltpu.VMEM((rows, width), jnp.float32)],
        cost_estimate=pl.CostEstimate(
            flops=2 * rows * inbox.shape[0] * width,
            bytes_accessed=2 * (2 * rows + inbox.shape[0]) * width,
            transcendentals=rows,
        ),
        name="finish",
    )(inbox, text, gain)


def per_device(hidden, proj_weight, proj_bias, route, text, norm_gain):
    replicas = lax.axis_size("dp")
    count, width = hidden.shape
    capacity = 2
    partner = lax.ppermute(hidden, "tensor", [(0, 1), (1, 0)])

    def everyone(block):
        mine = jnp.concatenate(
            [block, shift_x(block, 1), shift_x(block, 2), shift_x(block, -1)], axis=0
        )
        return jnp.concatenate([mine, swap_core(mine)], axis=0)

    bias = proj_bias[None, :]
    blocks = project(everyone(hidden), proj_weight, bias, False)
    blocks = project(everyone(partner), proj_weight, bias, True, blocks)
    own = lax.all_to_all(blocks, ("section", "tensor"), split_axis=0, concat_axis=0, tiled=True)
    outbox = pack(route, own, replicas * capacity)
    inbox = lax.all_to_all(
        outbox.reshape(replicas, capacity, width), "dp", split_axis=0, concat_axis=0, tiled=True
    )
    return finish(inbox.reshape(replicas * capacity, width), text, norm_gain[None, :])


def solution(mesh):
    in_specs = (
        P(("dp", "section", "tensor"), None),
        P(None, ("section", "tensor")),
        P(("section", "tensor")),
        P(("dp", "section", "tensor"), None),
        P(("dp", "section", "tensor"), None),
        P(),
    )
    out_specs = P(("dp", "section", "tensor"), None)
    return jax.shard_map(
        per_device, mesh=mesh, in_specs=in_specs, out_specs=out_specs, check_vma=False
    )
```

```python
import functools

import jax
import jax.numpy as jnp
from jax import lax
from jax.experimental import pallas as pl
from jax.experimental.pallas import tpu as pltpu
from jax.sharding import PartitionSpec as P


EMPTY = 2.0**100
NX = 4
GRANT = 16 * 1024 * 1024


def shift_x(block, by):
    n = lax.axis_size("section") // 2
    pairs = [(2 * x + c, 2 * ((x + by) % n) + c) for x in range(n) for c in range(2)]
    return lax.ppermute(block, "section", pairs)


def swap_core(block):
    n = lax.axis_size("section")
    return lax.ppermute(block, "section", [(i, i ^ 1) for i in range(n)])


def project_kernel(partner, swapped, lhs_ref, w_ref, bias_ref, *rest):
    out_ref, acc = rest[-2:]
    depth = lhs_ref.shape[1]
    step = 1024
    acc[...] = jnp.zeros_like(acc)

    @pl.loop(0, depth // step)
    def _(k):
        at = pl.ds(pl.multiple_of(k * step, step), step)
        acc[...] += jnp.dot(lhs_ref[:, at], w_ref[at, :], preferred_element_type=jnp.float32)

    if len(rest) == 3:
        out_ref[...] = rest[0][...]
    section = lax.axis_index("section")
    tensor = lax.axis_index("tensor")
    x, core = section // 2, section % 2
    t = (1 - tensor) if partner else tensor
    c = (1 - core) if swapped else core
    rows = out_ref.shape[1]
    bias = bias_ref[...].astype(jnp.float32)
    for k in range(NX):
        dst = (lax.rem(x - k + NX, NX) * 2 + c) * 2 + t
        out_ref[dst] = (acc[k * rows : (k + 1) * rows, :] + bias).astype(out_ref.dtype)


def project(lhs, weight, bias, partner, swapped, base=None):
    rows, depth = lhs.shape
    width = weight.shape[1]
    operands = [lhs, weight, bias] + ([] if base is None else [base])
    return pl.pallas_call(
        functools.partial(project_kernel, partner, swapped),
        in_specs=[pl.BlockSpec(memory_space=pltpu.VMEM)] * len(operands),
        out_specs=pl.BlockSpec(memory_space=pltpu.VMEM),
        out_shape=jax.ShapeDtypeStruct((4 * NX, rows // NX, width), jnp.bfloat16),
        scratch_shapes=[pltpu.VMEM((rows, width), jnp.float32)],
        compiler_params=pltpu.CompilerParams(vmem_limit_bytes=GRANT),
        cost_estimate=pl.CostEstimate(
            flops=2 * rows * depth * width,
            bytes_accessed=2 * (rows * depth + depth * width + rows * width),
            transcendentals=0,
        ),
        name="project",
    )(*operands)


def pack_kernel(route_ref, tokens_ref, out_ref):
    blocks, rows, width = tokens_ref.shape
    slots = out_ref.shape[0]
    first = lax.broadcasted_iota(jnp.int32, (rows, rows), 0)
    second = lax.broadcasted_iota(jnp.int32, (rows, rows), 1)
    down = route_ref[...].astype(jnp.float32)
    across = jnp.sum(jnp.where(first == second, down, 0.0), axis=0, keepdims=True)
    earlier = jnp.where((first < second) & (down == across), 1.0, 0.0)
    slot = 2.0 * across + jnp.sum(earlier, axis=0, keepdims=True)
    ids = lax.broadcasted_iota(jnp.int32, (slots, rows), 0).astype(jnp.float32)
    pick = jnp.where(ids == slot, 1.0, 0.0)
    mark = jnp.where(jnp.sum(pick, axis=1, keepdims=True) > 0.0, 0.0, EMPTY)
    pick = pick.astype(jnp.bfloat16)
    for k in range(blocks):
        moved = jnp.dot(pick, tokens_ref[k], preferred_element_type=jnp.float32)
        out_ref[:, k * width : (k + 1) * width] = (moved + mark).astype(out_ref.dtype)


def pack(route, tokens, slots):
    blocks, rows, width = tokens.shape
    return pl.pallas_call(
        pack_kernel,
        in_specs=[pl.BlockSpec(memory_space=pltpu.VMEM)] * 2,
        out_specs=pl.BlockSpec(memory_space=pltpu.VMEM),
        out_shape=jax.ShapeDtypeStruct((slots, blocks * width), jnp.bfloat16),
        cost_estimate=pl.CostEstimate(
            flops=2 * slots * rows * blocks * width,
            bytes_accessed=2 * (slots + rows) * blocks * width,
            transcendentals=0,
        ),
        compiler_params=pltpu.CompilerParams(vmem_limit_bytes=GRANT),
        name="pack",
    )(route, tokens)


def finish_kernel(inbox_ref, text_ref, gain_ref, out_ref, merged):
    slots, width = inbox_ref.shape
    rows = text_ref.shape[0]
    first = lax.broadcasted_iota(jnp.int32, (slots, slots), 0)
    second = lax.broadcasted_iota(jnp.int32, (slots, slots), 1)
    down = jnp.where(inbox_ref[:, 0:128].astype(jnp.float32)[:, 0:1] < EMPTY / 2, 1.0, 0.0)
    across = jnp.sum(jnp.where(first == second, down, 0.0), axis=0, keepdims=True)
    place = jnp.sum(jnp.where(first < second, down, 0.0), axis=0, keepdims=True)
    ids = lax.broadcasted_iota(jnp.int32, (rows, slots), 0).astype(jnp.float32)
    pick = jnp.where((ids == place) & (across > 0.0), 1.0, 0.0)
    is_image = jnp.sum(pick, axis=1, keepdims=True) > 0.0
    pick = pick.astype(jnp.bfloat16)
    step = 1024
    square = jnp.zeros((rows, 1), jnp.float32)
    for k in range(width // step):
        at = slice(k * step, (k + 1) * step)
        moved = jnp.dot(pick, inbox_ref[:, at], preferred_element_type=jnp.float32)
        values = jnp.where(is_image, moved, text_ref[:, at].astype(jnp.float32))
        merged[:, at] = values
        square += jnp.sum(values * values, axis=1, keepdims=True)
    scale_inv = lax.rsqrt(square * (1.0 / width) + 1e-05)
    for k in range(width // step):
        at = slice(k * step, (k + 1) * step)
        gain = gain_ref[:, at].astype(jnp.float32)
        out_ref[:, at] = (merged[:, at] * scale_inv * gain).astype(out_ref.dtype)


def finish(inbox, text, gain):
    rows, width = text.shape
    return pl.pallas_call(
        finish_kernel,
        in_specs=[pl.BlockSpec(memory_space=pltpu.VMEM)] * 3,
        out_specs=pl.BlockSpec(memory_space=pltpu.VMEM),
        out_shape=jax.ShapeDtypeStruct((rows, width), jnp.bfloat16),
        scratch_shapes=[pltpu.VMEM((rows, width), jnp.float32)],
        cost_estimate=pl.CostEstimate(
            flops=2 * rows * inbox.shape[0] * width,
            bytes_accessed=2 * (2 * rows + inbox.shape[0]) * width,
            transcendentals=rows,
        ),
        compiler_params=pltpu.CompilerParams(vmem_limit_bytes=GRANT),
        name="finish",
    )(inbox, text, gain)


def per_device(hidden, proj_weight, proj_bias, route, text, norm_gain):
    replicas = lax.axis_size("dp")
    _, width = hidden.shape
    capacity = 2
    bias = proj_bias[None, :]
    partner = lax.ppermute(hidden, "tensor", [(0, 1), (1, 0)])

    def along_x(block):
        pieces = [block]
        for by in (1, 2, -1):
            pieces.append(shift_x(block, by))
        return jnp.concatenate(pieces, axis=0)

    blocks = None
    for name, block in (("own", hidden), ("other", partner)):
        mine = along_x(block)
        blocks = project(mine, proj_weight, bias, name == "other", False, blocks)
        theirs = swap_core(mine)
        blocks = project(theirs, proj_weight, bias, name == "other", True, blocks)
    own = lax.all_to_all(blocks, ("section", "tensor"), split_axis=0, concat_axis=0, tiled=True)
    outbox = pack(route, own, replicas * capacity)
    inbox = lax.all_to_all(
        outbox.reshape(replicas, capacity, width), "dp", split_axis=0, concat_axis=0, tiled=True
    )
    return finish(inbox.reshape(replicas * capacity, width), text, norm_gain[None, :])


def solution(mesh):
    in_specs = (
        P(("dp", "section", "tensor"), None),
        P(None, ("section", "tensor")),
        P(("section", "tensor")),
        P(("dp", "section", "tensor"), None),
        P(("dp", "section", "tensor"), None),
        P(),
    )
    out_specs = P(("dp", "section", "tensor"), None)
    return jax.shard_map(
        per_device, mesh=mesh, in_specs=in_specs, out_specs=out_specs, check_vma=False
    )
```

```python
import functools

import jax
import jax.numpy as jnp
from jax import lax
from jax.experimental import pallas as pl
from jax.experimental.pallas import tpu as pltpu
from jax.sharding import PartitionSpec as P


EMPTY = 2.0**100
NX = 4
GRANT = 16 * 1024 * 1024


def shift_x(block, by):
    n = lax.axis_size("section") // 2
    pairs = [(2 * x + c, 2 * ((x + by) % n) + c) for x in range(n) for c in range(2)]
    return lax.ppermute(block, "section", pairs)


def swap_core(block):
    n = lax.axis_size("section")
    return lax.ppermute(block, "section", [(i, i ^ 1) for i in range(n)])


def project_kernel(partner, swapped, lhs_ref, w_ref, bias_ref, *rest):
    out_ref, acc = rest[-2:]
    depth = lhs_ref.shape[1]
    step = 1024
    acc[...] = jnp.zeros_like(acc)

    @pl.loop(0, depth // step)
    def _(k):
        at = pl.ds(pl.multiple_of(k * step, step), step)
        acc[...] += jnp.dot(lhs_ref[:, at], w_ref[at, :], preferred_element_type=jnp.float32)

    if len(rest) == 3:
        out_ref[...] = rest[0][...]
    section = lax.axis_index("section")
    tensor = lax.axis_index("tensor")
    x, core = section // 2, section % 2
    t = (1 - tensor) if partner else tensor
    c = (1 - core) if swapped else core
    rows = out_ref.shape[1]
    bias = bias_ref[...].astype(jnp.float32)
    for k in range(NX):
        dst = (lax.rem(x - k + NX, NX) * 2 + c) * 2 + t
        out_ref[dst] = (acc[k * rows : (k + 1) * rows, :] + bias).astype(out_ref.dtype)


def project(lhs, weight, bias, partner, swapped, base=None):
    rows, depth = lhs.shape
    width = weight.shape[1]
    operands = [lhs, weight, bias] + ([] if base is None else [base])
    return pl.pallas_call(
        functools.partial(project_kernel, partner, swapped),
        in_specs=[pl.BlockSpec(memory_space=pltpu.VMEM)] * len(operands),
        out_specs=pl.BlockSpec(memory_space=pltpu.VMEM),
        out_shape=jax.ShapeDtypeStruct((4 * NX, rows // NX, width), jnp.bfloat16),
        scratch_shapes=[pltpu.VMEM((rows, width), jnp.float32)],
        compiler_params=pltpu.CompilerParams(vmem_limit_bytes=GRANT),
        cost_estimate=pl.CostEstimate(
            flops=2 * rows * depth * width,
            bytes_accessed=2 * (rows * depth + depth * width + rows * width),
            transcendentals=0,
        ),
        name="project",
    )(*operands)


def pack_kernel(route_ref, tokens_ref, out_ref):
    blocks, rows, width = tokens_ref.shape
    replicas, capacity, _ = out_ref.shape
    slots = replicas * capacity
    first = lax.broadcasted_iota(jnp.int32, (rows, rows), 0)
    second = lax.broadcasted_iota(jnp.int32, (rows, rows), 1)
    down = route_ref[...].astype(jnp.float32)
    across = jnp.sum(jnp.where(first == second, down, 0.0), axis=0, keepdims=True)
    earlier = jnp.where((first < second) & (down == across), 1.0, 0.0)
    slot = 2.0 * across + jnp.sum(earlier, axis=0, keepdims=True)
    ids = lax.broadcasted_iota(jnp.int32, (slots, rows), 0).astype(jnp.float32)
    pick = jnp.where(ids == slot, 1.0, 0.0)
    mark = jnp.where(jnp.sum(pick, axis=1, keepdims=True) > 0.0, 0.0, EMPTY)
    pick = pick.astype(jnp.bfloat16)
    for k in range(blocks):
        moved = jnp.dot(pick, tokens_ref[k], preferred_element_type=jnp.float32)
        moved = (moved + mark).astype(out_ref.dtype)
        out_ref[:, :, k * width : (k + 1) * width] = moved.reshape(replicas, capacity, width)


def pack(route, tokens, replicas, capacity):
    blocks, rows, width = tokens.shape
    slots = replicas * capacity
    return pl.pallas_call(
        pack_kernel,
        in_specs=[pl.BlockSpec(memory_space=pltpu.VMEM)] * 2,
        out_specs=pl.BlockSpec(memory_space=pltpu.VMEM),
        out_shape=jax.ShapeDtypeStruct((replicas, capacity, blocks * width), jnp.bfloat16),
        cost_estimate=pl.CostEstimate(
            flops=2 * slots * rows * blocks * width,
            bytes_accessed=2 * (slots + rows) * blocks * width,
            transcendentals=0,
        ),
        compiler_params=pltpu.CompilerParams(vmem_limit_bytes=GRANT),
        name="pack",
    )(route, tokens)


def finish_kernel(inbox_ref, text_ref, gain_ref, out_ref, merged):
    slots, width = inbox_ref.shape[0] * inbox_ref.shape[1], inbox_ref.shape[2]
    rows = text_ref.shape[0]
    first = lax.broadcasted_iota(jnp.int32, (slots, slots), 0)
    second = lax.broadcasted_iota(jnp.int32, (slots, slots), 1)
    head = inbox_ref[:, :, 0:128].reshape(slots, 128).astype(jnp.float32)
    down = jnp.where(head[:, 0:1] < EMPTY / 2, 1.0, 0.0)
    across = jnp.sum(jnp.where(first == second, down, 0.0), axis=0, keepdims=True)
    place = jnp.sum(jnp.where(first < second, down, 0.0), axis=0, keepdims=True)
    ids = lax.broadcasted_iota(jnp.int32, (rows, slots), 0).astype(jnp.float32)
    pick = jnp.where((ids == place) & (across > 0.0), 1.0, 0.0)
    is_image = jnp.sum(pick, axis=1, keepdims=True) > 0.0
    pick = pick.astype(jnp.bfloat16)
    step = 1024
    square = jnp.zeros((rows, 1), jnp.float32)
    for k in range(width // step):
        at = slice(k * step, (k + 1) * step)
        arrived = inbox_ref[:, :, at].reshape(slots, step)
        moved = jnp.dot(pick, arrived, preferred_element_type=jnp.float32)
        values = jnp.where(is_image, moved, text_ref[:, at].astype(jnp.float32))
        merged[:, at] = values
        square += jnp.sum(values * values, axis=1, keepdims=True)
    scale_inv = lax.rsqrt(square * (1.0 / width) + 1e-05)
    for k in range(width // step):
        at = slice(k * step, (k + 1) * step)
        gain = gain_ref[:, at].astype(jnp.float32)
        out_ref[:, at] = (merged[:, at] * scale_inv * gain).astype(out_ref.dtype)


def finish(inbox, text, gain):
    rows, width = text.shape
    return pl.pallas_call(
        finish_kernel,
        in_specs=[pl.BlockSpec(memory_space=pltpu.VMEM)] * 3,
        out_specs=pl.BlockSpec(memory_space=pltpu.VMEM),
        out_shape=jax.ShapeDtypeStruct((rows, width), jnp.bfloat16),
        scratch_shapes=[pltpu.VMEM((rows, width), jnp.float32)],
        cost_estimate=pl.CostEstimate(
            flops=4 * rows * inbox.shape[0] * width,
            bytes_accessed=2 * (2 * rows + 2 * inbox.shape[0]) * width,
            transcendentals=rows,
        ),
        compiler_params=pltpu.CompilerParams(vmem_limit_bytes=GRANT),
        name="finish",
    )(inbox, text, gain)


def per_device(hidden, proj_weight, proj_bias, route, text, norm_gain):
    replicas = lax.axis_size("dp")
    capacity = 2
    bias = proj_bias[None, :]
    partner = lax.ppermute(hidden, "tensor", [(0, 1), (1, 0)])

    def along_x(block):
        pieces = [block]
        for by in (1, 2, -1):
            pieces.append(shift_x(block, by))
        return jnp.concatenate(pieces, axis=0)

    blocks = None
    for name, block in (("own", hidden), ("other", partner)):
        mine = along_x(block)
        blocks = project(mine, proj_weight, bias, name == "other", False, blocks)
        theirs = swap_core(mine)
        blocks = project(theirs, proj_weight, bias, name == "other", True, blocks)
    own = lax.all_to_all(blocks, ("section", "tensor"), split_axis=0, concat_axis=0, tiled=True)
    outbox = pack(route, own, replicas, capacity)
    inbox = lax.all_to_all(
        outbox, "dp", split_axis=0, concat_axis=0, tiled=True
    )
    return finish(inbox, text, norm_gain[None, :])


def solution(mesh):
    in_specs = (
        P(("dp", "section", "tensor"), None),
        P(None, ("section", "tensor")),
        P(("section", "tensor")),
        P(("dp", "section", "tensor"), None),
        P(("dp", "section", "tensor"), None),
        P(),
    )
    out_specs = P(("dp", "section", "tensor"), None)
    return jax.shard_map(
        per_device, mesh=mesh, in_specs=in_specs, out_specs=out_specs, check_vma=False
    )
```

```python
import functools

import jax
import jax.numpy as jnp
from jax import lax
from jax.experimental import pallas as pl
from jax.experimental.pallas import tpu as pltpu
from jax.sharding import PartitionSpec as P


NX = 4
GRANT = 16 * 1024 * 1024


def shift_x(block, by):
    n = lax.axis_size("section") // 2
    pairs = [(2 * x + c, 2 * ((x + by) % n) + c) for x in range(n) for c in range(2)]
    return lax.ppermute(block, "section", pairs)


def swap_core(block):
    n = lax.axis_size("section")
    return lax.ppermute(block, "section", [(i, i ^ 1) for i in range(n)])


def project_kernel(partner, swapped, lhs_ref, w_ref, bias_ref, *rest):
    out_ref, acc = rest[-2:]
    depth = lhs_ref.shape[1]
    step = 1024
    acc[...] = jnp.zeros_like(acc)

    @pl.loop(0, depth // step)
    def _(k):
        at = pl.ds(pl.multiple_of(k * step, step), step)
        acc[...] += jnp.dot(lhs_ref[:, at], w_ref[at, :], preferred_element_type=jnp.float32)

    if len(rest) == 3:
        out_ref[...] = rest[0][...]
    section = lax.axis_index("section")
    tensor = lax.axis_index("tensor")
    x, core = section // 2, section % 2
    t = (1 - tensor) if partner else tensor
    c = (1 - core) if swapped else core
    rows = out_ref.shape[1]
    bias = bias_ref[...].astype(jnp.float32)
    for k in range(NX):
        dst = (lax.rem(x - k + NX, NX) * 2 + c) * 2 + t
        out_ref[dst] = (acc[k * rows : (k + 1) * rows, :] + bias).astype(out_ref.dtype)


def project(lhs, weight, bias, partner, swapped, base=None):
    rows, depth = lhs.shape
    width = weight.shape[1]
    operands = [lhs, weight, bias] + ([] if base is None else [base])
    return pl.pallas_call(
        functools.partial(project_kernel, partner, swapped),
        in_specs=[pl.BlockSpec(memory_space=pltpu.VMEM)] * len(operands),
        out_specs=pl.BlockSpec(memory_space=pltpu.VMEM),
        out_shape=jax.ShapeDtypeStruct((4 * NX, rows // NX, width), jnp.bfloat16),
        scratch_shapes=[pltpu.VMEM((rows, width), jnp.float32)],
        compiler_params=pltpu.CompilerParams(vmem_limit_bytes=GRANT),
        cost_estimate=pl.CostEstimate(
            flops=2 * rows * depth * width,
            bytes_accessed=2 * (rows * depth + depth * width + rows * width),
            transcendentals=0,
        ),
        name="project",
    )(*operands)


def count_kernel(route_ref, out_ref):
    rows = route_ref.shape[0]
    replicas, _, lanes = out_ref.shape
    first = lax.broadcasted_iota(jnp.int32, (rows, rows), 0)
    second = lax.broadcasted_iota(jnp.int32, (rows, rows), 1)
    down = route_ref[...].astype(jnp.float32)
    across = jnp.sum(jnp.where(first == second, down, 0.0), axis=0, keepdims=True)
    ids = lax.broadcasted_iota(jnp.int32, (replicas, rows), 0).astype(jnp.float32)
    counts = jnp.sum(jnp.where(ids == across, 1.0, 0.0), axis=1, keepdims=True)
    counts = jnp.broadcast_to(counts, (replicas, lanes)).astype(jnp.int32)
    out_ref[...] = counts.reshape(replicas, 1, lanes)


def count(route, replicas):
    return pl.pallas_call(
        count_kernel,
        in_specs=[pl.BlockSpec(memory_space=pltpu.VMEM)],
        out_specs=pl.BlockSpec(memory_space=pltpu.VMEM),
        out_shape=jax.ShapeDtypeStruct((replicas, 1, 128), jnp.int32),
        compiler_params=pltpu.CompilerParams(vmem_limit_bytes=GRANT),
        name="count",
    )(route)


def pack_kernel(route_ref, tokens_ref, out_ref):
    blocks, rows, width = tokens_ref.shape
    replicas, capacity, _ = out_ref.shape
    slots = replicas * capacity
    first = lax.broadcasted_iota(jnp.int32, (rows, rows), 0)
    second = lax.broadcasted_iota(jnp.int32, (rows, rows), 1)
    down = route_ref[...].astype(jnp.float32)
    across = jnp.sum(jnp.where(first == second, down, 0.0), axis=0, keepdims=True)
    earlier = jnp.where((first < second) & (down == across), 1.0, 0.0)
    slot = 2.0 * across + jnp.sum(earlier, axis=0, keepdims=True)
    ids = lax.broadcasted_iota(jnp.int32, (slots, rows), 0).astype(jnp.float32)
    pick = jnp.where(ids == slot, 1.0, 0.0)
    pick = pick.astype(jnp.bfloat16)
    for k in range(blocks):
        moved = jnp.dot(pick, tokens_ref[k], preferred_element_type=jnp.float32)
        moved = moved.astype(out_ref.dtype).reshape(replicas, capacity, width)
        out_ref[:, :, k * width : (k + 1) * width] = moved


def pack(route, tokens, replicas, capacity):
    blocks, rows, width = tokens.shape
    slots = replicas * capacity
    return pl.pallas_call(
        pack_kernel,
        in_specs=[pl.BlockSpec(memory_space=pltpu.VMEM)] * 2,
        out_specs=pl.BlockSpec(memory_space=pltpu.VMEM),
        out_shape=jax.ShapeDtypeStruct((replicas, capacity, blocks * width), jnp.bfloat16),
        cost_estimate=pl.CostEstimate(
            flops=2 * slots * rows * blocks * width,
            bytes_accessed=2 * (slots + rows) * blocks * width,
            transcendentals=0,
        ),
        compiler_params=pltpu.CompilerParams(vmem_limit_bytes=GRANT),
        name="pack",
    )(route, tokens)


def finish_kernel(counts_ref, inbox_ref, text_ref, gain_ref, out_ref, merged):
    replicas, capacity, width = inbox_ref.shape
    slots = replicas * capacity
    rows = text_ref.shape[0]
    first = lax.broadcasted_iota(jnp.int32, (slots, slots), 0)
    second = lax.broadcasted_iota(jnp.int32, (slots, slots), 1)
    counts = counts_ref[...].reshape(replicas, 128).astype(jnp.float32)[:, 0:1]
    same = lax.broadcasted_iota(jnp.int32, (replicas, replicas), 0) == (
        lax.broadcasted_iota(jnp.int32, (replicas, replicas), 1)
    )
    counts = jnp.sum(jnp.where(same, counts, 0.0), axis=0, keepdims=True)
    place_in = lax.broadcasted_iota(jnp.int32, (slots, replicas), 0) - (
        capacity * lax.broadcasted_iota(jnp.int32, (slots, replicas), 1)
    )
    held = (place_in >= 0) & (place_in < capacity) & (place_in.astype(jnp.float32) < counts)
    down = jnp.sum(jnp.where(held, 1.0, 0.0), axis=1, keepdims=True)
    across = jnp.sum(jnp.where(first == second, down, 0.0), axis=0, keepdims=True)
    place = jnp.sum(jnp.where(first < second, down, 0.0), axis=0, keepdims=True)
    ids = lax.broadcasted_iota(jnp.int32, (rows, slots), 0).astype(jnp.float32)
    pick = jnp.where((ids == place) & (across > 0.0), 1.0, 0.0)
    is_image = jnp.sum(pick, axis=1, keepdims=True) > 0.0
    pick = pick.astype(jnp.bfloat16)
    step = 1024
    square = jnp.zeros((rows, 1), jnp.float32)
    for k in range(width // step):
        at = slice(k * step, (k + 1) * step)
        arrived = inbox_ref[:, :, at].reshape(slots, step)
        moved = jnp.dot(pick, arrived, preferred_element_type=jnp.float32)
        values = jnp.where(is_image, moved, text_ref[:, at].astype(jnp.float32))
        merged[:, at] = values
        square += jnp.sum(values * values, axis=1, keepdims=True)
    scale_inv = lax.rsqrt(square * (1.0 / width) + 1e-05)
    for k in range(width // step):
        at = slice(k * step, (k + 1) * step)
        gain = gain_ref[:, at].astype(jnp.float32)
        out_ref[:, at] = (merged[:, at] * scale_inv * gain).astype(out_ref.dtype)


def finish(counts, inbox, text, gain):
    rows, width = text.shape
    return pl.pallas_call(
        finish_kernel,
        in_specs=[pl.BlockSpec(memory_space=pltpu.VMEM)] * 4,
        out_specs=pl.BlockSpec(memory_space=pltpu.VMEM),
        out_shape=jax.ShapeDtypeStruct((rows, width), jnp.bfloat16),
        scratch_shapes=[pltpu.VMEM((rows, width), jnp.float32)],
        cost_estimate=pl.CostEstimate(
            flops=4 * rows * inbox.shape[0] * width,
            bytes_accessed=2 * (2 * rows + 2 * inbox.shape[0]) * width,
            transcendentals=rows,
        ),
        compiler_params=pltpu.CompilerParams(vmem_limit_bytes=GRANT),
        name="finish",
    )(counts, inbox, text, gain)


def per_device(hidden, proj_weight, proj_bias, route, text, norm_gain):
    replicas = lax.axis_size("dp")
    capacity = 2
    bias = proj_bias[None, :]
    partner = lax.ppermute(hidden, "tensor", [(0, 1), (1, 0)])

    counts = lax.all_to_all(count(route, replicas), "dp", split_axis=0, concat_axis=0, tiled=True)

    def along_x(block):
        pieces = [block]
        for by in (1, 2, -1):
            pieces.append(shift_x(block, by))
        return jnp.concatenate(pieces, axis=0)

    blocks = None
    for name, block in (("own", hidden), ("other", partner)):
        mine = along_x(block)
        blocks = project(mine, proj_weight, bias, name == "other", False, blocks)
        theirs = swap_core(mine)
        blocks = project(theirs, proj_weight, bias, name == "other", True, blocks)
    own = lax.all_to_all(blocks, ("section", "tensor"), split_axis=0, concat_axis=0, tiled=True)
    outbox = pack(route, own, replicas, capacity)
    inbox = lax.all_to_all(
        outbox, "dp", split_axis=0, concat_axis=0, tiled=True
    )
    return finish(counts, inbox, text, norm_gain[None, :])


def solution(mesh):
    in_specs = (
        P(("dp", "section", "tensor"), None),
        P(None, ("section", "tensor")),
        P(("section", "tensor")),
        P(("dp", "section", "tensor"), None),
        P(("dp", "section", "tensor"), None),
        P(),
    )
    out_specs = P(("dp", "section", "tensor"), None)
    return jax.shard_map(
        per_device, mesh=mesh, in_specs=in_specs, out_specs=out_specs, check_vma=False
    )
```

```python
import functools

import jax
import jax.numpy as jnp
from jax import lax
from jax.experimental import pallas as pl
from jax.experimental.pallas import tpu as pltpu
from jax.sharding import PartitionSpec as P


EMPTY = 2.0**100
NX = 4
GRANT = 16 * 1024 * 1024


def shift_x(block, by):
    n = lax.axis_size("section") // 2
    pairs = [(2 * x + c, 2 * ((x + by) % n) + c) for x in range(n) for c in range(2)]
    return lax.ppermute(block, "section", pairs)


def swap_core(block):
    n = lax.axis_size("section")
    return lax.ppermute(block, "section", [(i, i ^ 1) for i in range(n)])


def project_kernel(partner, swapped, lhs_ref, w_ref, bias_ref, *rest):
    out_ref, acc = rest[-2:]
    depth = lhs_ref.shape[1]
    step = 1024
    acc[...] = jnp.zeros_like(acc)

    @pl.loop(0, depth // step)
    def _(k):
        at = pl.ds(pl.multiple_of(k * step, step), step)
        acc[...] += jnp.dot(lhs_ref[:, at], w_ref[at, :], preferred_element_type=jnp.float32)

    if len(rest) == 3:
        out_ref[...] = rest[0][...]
    section = lax.axis_index("section")
    tensor = lax.axis_index("tensor")
    x, core = section // 2, section % 2
    t = (1 - tensor) if partner else tensor
    c = (1 - core) if swapped else core
    rows = out_ref.shape[1]
    bias = bias_ref[...].astype(jnp.float32)
    for k in range(NX):
        dst = (lax.rem(x - k + NX, NX) * 2 + c) * 2 + t
        out_ref[dst] = (acc[k * rows : (k + 1) * rows, :] + bias).astype(out_ref.dtype)


def project(lhs, weight, bias, partner, swapped, base=None):
    rows, depth = lhs.shape
    width = weight.shape[1]
    operands = [lhs, weight, bias] + ([] if base is None else [base])
    return pl.pallas_call(
        functools.partial(project_kernel, partner, swapped),
        in_specs=[pl.BlockSpec(memory_space=pltpu.VMEM)] * len(operands),
        out_specs=pl.BlockSpec(memory_space=pltpu.VMEM),
        out_shape=jax.ShapeDtypeStruct((4 * NX, rows // NX, width), jnp.bfloat16),
        scratch_shapes=[pltpu.VMEM((rows, width), jnp.float32)],
        compiler_params=pltpu.CompilerParams(vmem_limit_bytes=GRANT),
        cost_estimate=pl.CostEstimate(
            flops=2 * rows * depth * width,
            bytes_accessed=2 * (rows * depth + depth * width + rows * width),
            transcendentals=0,
        ),
        name="project",
    )(*operands)


def prepare_kernel(route_ref, gain_ref, slot_ref, wide_ref):
    rows = route_ref.shape[1]
    first = lax.broadcasted_iota(jnp.int32, (rows, rows), 0)
    second = lax.broadcasted_iota(jnp.int32, (rows, rows), 1)
    across = route_ref[...].astype(jnp.float32)
    down = jnp.sum(jnp.where(first == second, across, 0.0), axis=1, keepdims=True)
    earlier = jnp.where((first < second) & (down == across), 1.0, 0.0)
    slot_ref[...] = 2.0 * across + jnp.sum(earlier, axis=0, keepdims=True)
    wide_ref[...] = gain_ref[...].astype(jnp.float32)


def prepare(route, gain):
    return pl.pallas_call(
        prepare_kernel,
        in_specs=[pl.BlockSpec(memory_space=pltpu.VMEM)] * 2,
        out_specs=[pl.BlockSpec(memory_space=pltpu.VMEM)] * 2,
        out_shape=[
            jax.ShapeDtypeStruct(route.shape, jnp.float32),
            jax.ShapeDtypeStruct(gain.shape, jnp.float32),
        ],
        compiler_params=pltpu.CompilerParams(vmem_limit_bytes=GRANT),
        name="prepare",
    )(route, gain)


def pack_kernel(slot_ref, tokens_ref, out_ref):
    blocks, rows, width = tokens_ref.shape
    replicas, capacity, _ = out_ref.shape
    slots = replicas * capacity
    slot = slot_ref[...]
    ids = lax.broadcasted_iota(jnp.int32, (slots, rows), 0).astype(jnp.float32)
    pick = jnp.where(ids == slot, 1.0, 0.0)
    mark = jnp.where(jnp.sum(pick, axis=1, keepdims=True) > 0.0, 0.0, EMPTY)
    pick = pick.astype(jnp.bfloat16)
    for k in range(blocks):
        moved = jnp.dot(pick, tokens_ref[k], preferred_element_type=jnp.float32)
        moved = (moved + mark).astype(out_ref.dtype)
        out_ref[:, :, k * width : (k + 1) * width] = moved.reshape(replicas, capacity, width)


def pack(slot, tokens, replicas, capacity):
    blocks, rows, width = tokens.shape
    slots = replicas * capacity
    return pl.pallas_call(
        pack_kernel,
        in_specs=[pl.BlockSpec(memory_space=pltpu.VMEM)] * 2,
        out_specs=pl.BlockSpec(memory_space=pltpu.VMEM),
        out_shape=jax.ShapeDtypeStruct((replicas, capacity, blocks * width), jnp.bfloat16),
        cost_estimate=pl.CostEstimate(
            flops=2 * slots * rows * blocks * width,
            bytes_accessed=2 * (slots + rows) * blocks * width,
            transcendentals=0,
        ),
        compiler_params=pltpu.CompilerParams(vmem_limit_bytes=GRANT),
        name="pack",
    )(slot, tokens)


def finish_kernel(inbox_ref, text_ref, gain_ref, out_ref, merged):
    slots, width = inbox_ref.shape[0] * inbox_ref.shape[1], inbox_ref.shape[2]
    rows = text_ref.shape[0]
    first = lax.broadcasted_iota(jnp.int32, (slots, slots), 0)
    second = lax.broadcasted_iota(jnp.int32, (slots, slots), 1)
    head = inbox_ref[:, :, 0:128].reshape(slots, 128).astype(jnp.float32)
    down = jnp.where(head[:, 0:1] < EMPTY / 2, 1.0, 0.0)
    across = jnp.sum(jnp.where(first == second, down, 0.0), axis=0, keepdims=True)
    place = jnp.sum(jnp.where(first < second, down, 0.0), axis=0, keepdims=True)
    ids = lax.broadcasted_iota(jnp.int32, (rows, slots), 0).astype(jnp.float32)
    pick = jnp.where((ids == place) & (across > 0.0), 1.0, 0.0)
    is_image = jnp.sum(pick, axis=1, keepdims=True) > 0.0
    pick = pick.astype(jnp.bfloat16)
    step = 1024
    square = jnp.zeros((rows, 1), jnp.float32)
    for k in range(width // step):
        at = slice(k * step, (k + 1) * step)
        arrived = inbox_ref[:, :, at].reshape(slots, step)
        moved = jnp.dot(pick, arrived, preferred_element_type=jnp.float32)
        values = jnp.where(is_image, moved, text_ref[:, at].astype(jnp.float32))
        merged[:, at] = values
        square += jnp.sum(values * values, axis=1, keepdims=True)
    scale_inv = lax.rsqrt(square * (1.0 / width) + 1e-05)
    for k in range(width // step):
        at = slice(k * step, (k + 1) * step)
        out_ref[:, at] = (merged[:, at] * scale_inv * gain_ref[:, at]).astype(out_ref.dtype)


def finish(inbox, text, gain):
    rows, width = text.shape
    return pl.pallas_call(
        finish_kernel,
        in_specs=[pl.BlockSpec(memory_space=pltpu.VMEM)] * 3,
        out_specs=pl.BlockSpec(memory_space=pltpu.VMEM),
        out_shape=jax.ShapeDtypeStruct((rows, width), jnp.bfloat16),
        scratch_shapes=[pltpu.VMEM((rows, width), jnp.float32)],
        cost_estimate=pl.CostEstimate(
            flops=4 * rows * inbox.shape[0] * width,
            bytes_accessed=2 * (2 * rows + 2 * inbox.shape[0]) * width,
            transcendentals=rows,
        ),
        compiler_params=pltpu.CompilerParams(vmem_limit_bytes=GRANT),
        name="finish",
    )(inbox, text, gain)


def per_device(hidden, proj_weight, proj_bias, route, text, norm_gain):
    replicas = lax.axis_size("dp")
    capacity = 2
    bias = proj_bias[None, :]
    partner = lax.ppermute(hidden, "tensor", [(0, 1), (1, 0)])

    slot, gain = prepare(route.reshape(1, -1), norm_gain[None, :])

    def along_x(block):
        pieces = [block]
        for by in (1, 2, -1):
            pieces.append(shift_x(block, by))
        return jnp.concatenate(pieces, axis=0)

    blocks = None
    for name, block in (("own", hidden), ("other", partner)):
        mine = along_x(block)
        blocks = project(mine, proj_weight, bias, name == "other", False, blocks)
        theirs = swap_core(mine)
        blocks = project(theirs, proj_weight, bias, name == "other", True, blocks)
    own = lax.all_to_all(blocks, ("section", "tensor"), split_axis=0, concat_axis=0, tiled=True)
    outbox = pack(slot, own, replicas, capacity)
    inbox = lax.all_to_all(
        outbox, "dp", split_axis=0, concat_axis=0, tiled=True
    )
    return finish(inbox, text, gain)


def solution(mesh):
    in_specs = (
        P(("dp", "section", "tensor"), None),
        P(None, ("section", "tensor")),
        P(("section", "tensor")),
        P(("dp", "section", "tensor"), None),
        P(("dp", "section", "tensor"), None),
        P(),
    )
    out_specs = P(("dp", "section", "tensor"), None)
    return jax.shard_map(
        per_device, mesh=mesh, in_specs=in_specs, out_specs=out_specs, check_vma=False
    )
```

```python
import functools

import jax
import jax.numpy as jnp
from jax import lax
from jax.experimental import pallas as pl
from jax.experimental.pallas import tpu as pltpu
from jax.sharding import PartitionSpec as P


EMPTY = 2.0**100
NX = 4
GRANT = 16 * 1024 * 1024


def shift_x(block, by):
    n = lax.axis_size("section") // 2
    pairs = [(2 * x + c, 2 * ((x + by) % n) + c) for x in range(n) for c in range(2)]
    return lax.ppermute(block, "section", pairs)


def swap_core(block):
    n = lax.axis_size("section")
    return lax.ppermute(block, "section", [(i, i ^ 1) for i in range(n)])


def project_kernel(partner, swapped, lhs_ref, w_ref, bias_ref, *rest):
    out_ref, acc = rest[-2:]
    depth = lhs_ref.shape[1]
    step = 1024
    acc[...] = jnp.zeros_like(acc)

    @pl.loop(0, depth // step)
    def _(k):
        at = pl.ds(pl.multiple_of(k * step, step), step)
        acc[...] += jnp.dot(lhs_ref[:, at], w_ref[at, :], preferred_element_type=jnp.float32)

    if len(rest) == 3:
        out_ref[...] = rest[0][...]
    section = lax.axis_index("section")
    x, core = section // 2, section % 2
    c = (1 - core) if swapped else core
    rows = out_ref.shape[1]
    bias = bias_ref[...].astype(jnp.float32)
    for k in range(NX):
        from_x = lax.rem(x - k + NX, NX)
        dst = from_x if partner else from_x * 2 + c
        out_ref[dst] = (acc[k * rows : (k + 1) * rows, :] + bias).astype(out_ref.dtype)


def project(lhs, weight, bias, partner, swapped, base=None):
    rows, depth = lhs.shape
    width = weight.shape[1]
    operands = [lhs, weight, bias] + ([] if base is None else [base])
    blocks = NX if partner else 2 * NX
    return pl.pallas_call(
        functools.partial(project_kernel, partner, swapped),
        in_specs=[pl.BlockSpec(memory_space=pltpu.VMEM)] * len(operands),
        out_specs=pl.BlockSpec(memory_space=pltpu.VMEM),
        out_shape=jax.ShapeDtypeStruct((blocks, rows // NX, width), jnp.bfloat16),
        scratch_shapes=[pltpu.VMEM((rows, width), jnp.float32)],
        compiler_params=pltpu.CompilerParams(vmem_limit_bytes=GRANT),
        cost_estimate=pl.CostEstimate(
            flops=2 * rows * depth * width,
            bytes_accessed=2 * (rows * depth + depth * width + rows * width),
            transcendentals=0,
        ),
        name="project",
    )(*operands)


def join_kernel(own_ref, same_ref, swapped_ref, out_ref):
    core = lax.axis_index("section") % 2
    tensor = lax.axis_index("tensor")
    width = own_ref.shape[2]
    out_ref[:, :, pl.ds(pl.multiple_of(tensor * width, width), width)] = own_ref[...]
    rest = pl.ds(pl.multiple_of((1 - tensor) * width, width), width)
    for x in range(NX):
        out_ref[2 * x + core, :, rest] = same_ref[x]
        out_ref[2 * x + 1 - core, :, rest] = swapped_ref[x]


def join(own, same, swapped):
    blocks, rows, width = own.shape
    return pl.pallas_call(
        join_kernel,
        in_specs=[pl.BlockSpec(memory_space=pltpu.VMEM)] * 3,
        out_specs=pl.BlockSpec(memory_space=pltpu.VMEM),
        out_shape=jax.ShapeDtypeStruct((blocks, rows, 2 * width), own.dtype),
        compiler_params=pltpu.CompilerParams(vmem_limit_bytes=GRANT),
        name="join",
    )(own, same, swapped)


def prepare_kernel(route_ref, gain_ref, slot_ref, wide_ref):
    rows = route_ref.shape[1]
    first = lax.broadcasted_iota(jnp.int32, (rows, rows), 0)
    second = lax.broadcasted_iota(jnp.int32, (rows, rows), 1)
    across = route_ref[...].astype(jnp.float32)
    down = jnp.sum(jnp.where(first == second, across, 0.0), axis=1, keepdims=True)
    earlier = jnp.where((first < second) & (down == across), 1.0, 0.0)
    slot_ref[...] = 2.0 * across + jnp.sum(earlier, axis=0, keepdims=True)
    wide_ref[...] = gain_ref[...].astype(jnp.float32)


def prepare(route, gain):
    return pl.pallas_call(
        prepare_kernel,
        in_specs=[pl.BlockSpec(memory_space=pltpu.VMEM)] * 2,
        out_specs=[pl.BlockSpec(memory_space=pltpu.VMEM)] * 2,
        out_shape=[
            jax.ShapeDtypeStruct(route.shape, jnp.float32),
            jax.ShapeDtypeStruct(gain.shape, jnp.float32),
        ],
        compiler_params=pltpu.CompilerParams(vmem_limit_bytes=GRANT),
        name="prepare",
    )(route, gain)


def pack_kernel(slot_ref, tokens_ref, out_ref):
    blocks, rows, width = tokens_ref.shape
    replicas, capacity, _ = out_ref.shape
    slots = replicas * capacity
    slot = slot_ref[...]
    ids = lax.broadcasted_iota(jnp.int32, (slots, rows), 0).astype(jnp.float32)
    pick = jnp.where(ids == slot, 1.0, 0.0)
    mark = jnp.where(jnp.sum(pick, axis=1, keepdims=True) > 0.0, 0.0, EMPTY)
    pick = pick.astype(jnp.bfloat16)
    for k in range(blocks):
        moved = jnp.dot(pick, tokens_ref[k], preferred_element_type=jnp.float32)
        moved = (moved + mark).astype(out_ref.dtype)
        out_ref[:, :, k * width : (k + 1) * width] = moved.reshape(replicas, capacity, width)


def pack(slot, tokens, replicas, capacity):
    blocks, rows, width = tokens.shape
    slots = replicas * capacity
    return pl.pallas_call(
        pack_kernel,
        in_specs=[pl.BlockSpec(memory_space=pltpu.VMEM)] * 2,
        out_specs=pl.BlockSpec(memory_space=pltpu.VMEM),
        out_shape=jax.ShapeDtypeStruct((replicas, capacity, blocks * width), jnp.bfloat16),
        cost_estimate=pl.CostEstimate(
            flops=2 * slots * rows * blocks * width,
            bytes_accessed=2 * (slots + rows) * blocks * width,
            transcendentals=0,
        ),
        compiler_params=pltpu.CompilerParams(vmem_limit_bytes=GRANT),
        name="pack",
    )(slot, tokens)


def finish_kernel(inbox_ref, text_ref, gain_ref, out_ref, merged):
    slots, width = inbox_ref.shape[0] * inbox_ref.shape[1], inbox_ref.shape[2]
    rows = text_ref.shape[0]
    first = lax.broadcasted_iota(jnp.int32, (slots, slots), 0)
    second = lax.broadcasted_iota(jnp.int32, (slots, slots), 1)
    head = inbox_ref[:, :, 0:128].reshape(slots, 128).astype(jnp.float32)
    down = jnp.where(head[:, 0:1] < EMPTY / 2, 1.0, 0.0)
    across = jnp.sum(jnp.where(first == second, down, 0.0), axis=0, keepdims=True)
    place = jnp.sum(jnp.where(first < second, down, 0.0), axis=0, keepdims=True)
    ids = lax.broadcasted_iota(jnp.int32, (rows, slots), 0).astype(jnp.float32)
    pick = jnp.where((ids == place) & (across > 0.0), 1.0, 0.0)
    is_image = jnp.sum(pick, axis=1, keepdims=True) > 0.0
    pick = pick.astype(jnp.bfloat16)
    step = 1024
    square = jnp.zeros((rows, 1), jnp.float32)
    for k in range(width // step):
        at = slice(k * step, (k + 1) * step)
        arrived = inbox_ref[:, :, at].reshape(slots, step)
        moved = jnp.dot(pick, arrived, preferred_element_type=jnp.float32)
        values = jnp.where(is_image, moved, text_ref[:, at].astype(jnp.float32))
        merged[:, at] = values
        square += jnp.sum(values * values, axis=1, keepdims=True)
    scale_inv = lax.rsqrt(square * (1.0 / width) + 1e-05)
    for k in range(width // step):
        at = slice(k * step, (k + 1) * step)
        out_ref[:, at] = (merged[:, at] * scale_inv * gain_ref[:, at]).astype(out_ref.dtype)


def finish(inbox, text, gain):
    rows, width = text.shape
    return pl.pallas_call(
        finish_kernel,
        in_specs=[pl.BlockSpec(memory_space=pltpu.VMEM)] * 3,
        out_specs=pl.BlockSpec(memory_space=pltpu.VMEM),
        out_shape=jax.ShapeDtypeStruct((rows, width), jnp.bfloat16),
        scratch_shapes=[pltpu.VMEM((rows, width), jnp.float32)],
        cost_estimate=pl.CostEstimate(
            flops=4 * rows * inbox.shape[0] * width,
            bytes_accessed=2 * (2 * rows + 2 * inbox.shape[0]) * width,
            transcendentals=rows,
        ),
        compiler_params=pltpu.CompilerParams(vmem_limit_bytes=GRANT),
        name="finish",
    )(inbox, text, gain)


def per_device(hidden, proj_weight, proj_bias, route, text, norm_gain):
    replicas = lax.axis_size("dp")
    capacity = 2
    bias = proj_bias[None, :]
    partner = lax.ppermute(hidden, "tensor", [(0, 1), (1, 0)])

    slot, gain = prepare(route.reshape(1, -1), norm_gain[None, :])

    def along_x(block):
        pieces = [block]
        for by in (1, 2, -1):
            pieces.append(shift_x(block, by))
        return jnp.concatenate(pieces, axis=0)

    def send_back(block):
        return lax.ppermute(block, "tensor", [(0, 1), (1, 0)])

    mine = along_x(hidden)
    kept = project(mine, proj_weight, bias, False, False)
    theirs = swap_core(mine)
    kept = project(theirs, proj_weight, bias, False, True, kept)
    mine = along_x(partner)
    same = project(mine, proj_weight, bias, True, False)
    theirs = swap_core(mine)
    swapped = project(theirs, proj_weight, bias, True, True)
    blocks = join(kept, send_back(same), send_back(swapped))
    own = lax.all_to_all(blocks, "section", split_axis=0, concat_axis=0, tiled=True)
    outbox = pack(slot, own, replicas, capacity)
    inbox = lax.all_to_all(
        outbox, "dp", split_axis=0, concat_axis=0, tiled=True
    )
    return finish(inbox, text, gain)


def solution(mesh):
    in_specs = (
        P(("dp", "section", "tensor"), None),
        P(None, ("section", "tensor")),
        P(("section", "tensor")),
        P(("dp", "section", "tensor"), None),
        P(("dp", "section", "tensor"), None),
        P(),
    )
    out_specs = P(("dp", "section", "tensor"), None)
    return jax.shard_map(
        per_device, mesh=mesh, in_specs=in_specs, out_specs=out_specs, check_vma=False
    )
```
